512 devices in a mesh: gx: 32 (over y, x, core), gy: 16 (over z).
Axes of the slice: x: 4, y: 4, z: 16, core: 2. Of those that a mesh axis runs over, the one named last changes fastest.
Arguments:
- patches: bfloat16 [256, 8192], P('gy', 'gx'), may hold values from -400 to 400, as said below
- norm_gain: bfloat16 [8192], P('gx'), may hold values from 0.099609375 to 1.8984375
- gate_weight: bfloat16 [8192, 28672], P('gx', 'gy'), may hold values from -0.0625 to 0.0625
- up_weight: bfloat16 [8192, 28672], P('gx', 'gy'), may hold values from -0.0625 to 0.0625
- down_weight: bfloat16 [28672, 8192], P('gy', 'gx'), may hold values from -0.03125 to 0.03125
Outputs:
- block_out: bfloat16 [256, 8192], P('gy', 'gx')
The draws below stay inside these ranges and needn't reach their ends.
Inputs may be any that keep to these rules, and one draw needn't show every extreme that they name: `patches`: real-valued activations of a pooled encoder.
All inputs are finite; a program needn't handle non-finite values.
Results may differ from the reference program's by a relative error of at most 0.0065.
Values may be sent and summed in bfloat16 or wider, within the bound.
A program may use at most 64 MiB of HBM per device.

```python
import jax
import jax.numpy as jnp
from jax import lax

D = 8192
FF = 28672
TOK = 256


def draw_patches(key, part):
    keys = jax.random.split(jax.random.fold_in(key, 17), 3)
    offsets = jax.random.uniform(keys[1], (1, D), minval=-0.25, maxval=0.25)
    columns = 10.0 ** (0.5 * jnp.arange(D, dtype=jnp.float32)[None, :] / D + offsets)
    row_scale = 10.0 ** jax.random.uniform(keys[0], (TOK, 1))
    base = jnp.clip(jax.random.normal(keys[2], (TOK, D)), -6.0, 6.0)
    return (base * row_scale * columns).astype(jnp.bfloat16)


def block_scale(key, shape, cuts, smallest, high):
    factor_of = 1.0
    for position, shards_of in cuts:
        draws = jax.random.uniform(jax.random.fold_in(jax.random.fold_in(key, 6), position), (shards_of,), jnp.float32, smallest / len(cuts), high / len(cuts))
        factor_of = factor_of * jnp.repeat(jnp.exp(draws), shape[position] // shards_of).reshape((-1,) + (1,) * (len(shape) - 1 - position))
    return factor_of


def noise(own_key, dims, scale, most, cuts=(), kind=jnp.bfloat16):
    array = jax.random.normal(own_key, dims, jnp.float32) * scale
    if len(cuts) > 0:
        array = block_scale(own_key, dims, cuts, -0.22, 0.18) * array
    return jnp.clip(array, min=-most, max=most).astype(kind)


def setup_inputs(seed: int = 0) -> dict:
    streams_of = jax.random.split(jax.random.key(seed), 6)
    patches = draw_patches(jax.random.fold_in(streams_of[5], 71), 0)
    norm_gain = jnp.clip(1.0 + 0.18 * jax.random.normal(streams_of[1], (D,), jnp.float32), 0.099609375, 1.8984375).astype(jnp.bfloat16)
    gate_weight = noise(streams_of[2], (D, FF), D ** -0.5, 0.0625, ((0, 32), (1, 16)))
    up_weight = noise(streams_of[3], (D, FF), D ** -0.5, 0.0625, ((0, 32), (1, 16)))
    down_weight = noise(streams_of[4], (FF, D), FF ** -0.5, 0.03125, ((0, 16), (1, 32)))
    return dict(patches=patches, norm_gain=norm_gain, gate_weight=gate_weight, up_weight=up_weight, down_weight=down_weight)


EPS = 1e-05

def reference(patches, norm_gain, gate_weight, up_weight, down_weight):
    values = patches.astype(jnp.float32)
    mean_sq = lax.optimization_barrier(jnp.mean(values * values, axis=1))
    normed = (values * lax.rsqrt(mean_sq + EPS)[:, None] * norm_gain.astype(jnp.float32)[None, :]).astype(jnp.bfloat16)
    gate = jnp.dot(normed, gate_weight, preferred_element_type=jnp.float32)
    up = jnp.dot(normed, up_weight, preferred_element_type=jnp.float32)
    hidden = (jax.nn.silu(gate) * up).astype(jnp.bfloat16)
    return jnp.dot(hidden, down_weight, preferred_element_type=jnp.float32).astype(jnp.bfloat16)
```

```python
import functools

import jax
import jax.numpy as jnp
from jax import lax
from jax.experimental import pallas as pl
from jax.experimental.pallas import tpu as pltpu
from jax.sharding import Mesh
from jax.sharding import PartitionSpec as P

GX = ("gx_0", "gx_1", "gx_2")
EPS = 1e-05
MESH = pl.DeviceIdType.MESH

NZ = 16
TB = 16
DL = 256
FL = 1792
FH = FL // 2
NO = 16
GT = 128
OT = GT // NO
PW = FL + 128
NEAR = 4
HOME = 3


def place(rel):
    return (rel + HOME) % NZ


def kernel(
    x_hbm, gain_hbm, wg_hbm, wu_hbm, wd_hbm, out_ref,
    xb, gb, wgu, wd, pb, rb, hb, db, de, zs, zb,
    loc_sem, bar_w_send, bar_w_recv, x_send, x_recv, xd_send, xd_recv,
    p_send, p_recv, h_send, h_recv, d_send, d_recv, z_send, z_recv,
):
    y = lax.axis_index("gx_0")
    x = lax.axis_index("gx_1")
    c = lax.axis_index("gx_2")
    z = lax.axis_index("gy")
    other = 1 - c
    me = y * 4 + x
    partner = (y, x, other, z)

    def at_z(k):
        return (y, x, c, lax.rem(z + (k % NZ), NZ))

    def in_plane(d):
        return (lax.rem(y + d // 4, 4), lax.rem(x + d % 4, 4), c, z)

    own_half = pl.ds(pl.multiple_of(c * FH, 128), FH)
    other_half = pl.ds(pl.multiple_of(other * FH, 128), FH)
    own_d = pl.ds(pl.multiple_of(c * DL, 256), DL)
    loads = [
        pltpu.make_async_copy(x_hbm, xb.at[c, HOME * TB : (HOME + 1) * TB], loc_sem.at[0]),
        pltpu.make_async_copy(gain_hbm, gb.at[own_d], loc_sem.at[1]),
        pltpu.make_async_copy(wg_hbm.at[:, own_half], wgu.at[own_d, 0:FH], loc_sem.at[2]),
        pltpu.make_async_copy(wu_hbm.at[:, own_half], wgu.at[own_d, FH:FL], loc_sem.at[3]),
        pltpu.make_async_copy(wd_hbm.at[own_half, :], wd.at[:, own_d], loc_sem.at[4]),
    ]
    for copy in loads:
        copy.start()

    barrier = pltpu.get_barrier_semaphore()
    peers = [at_z(k) for k in range(-NEAR, NEAR + 1) if k != 0]
    peers += [in_plane(d) for d in range(1, NO)]
    peers += [partner]
    for peer in peers:
        pl.semaphore_signal(barrier, inc=1, device_id=peer, device_id_type=MESH)
    loads[0].wait()
    pl.semaphore_wait(barrier, len(peers))

    def block(rel):
        p = place(rel)
        return xb.at[c, p * TB : (p + 1) * TB]

    def send_x(src_rel, k, index):
        return pltpu.make_async_remote_copy(
            src_ref=block(src_rel),
            dst_ref=block(src_rel - k),
            send_sem=x_send.at[index],
            recv_sem=x_recv.at[(src_rel - k) % NZ],
            device_id=at_z(k),
            device_id_type=MESH,
        )

    def arrive_x(rel):
        pltpu.make_async_remote_copy(
            src_ref=block(rel),
            dst_ref=block(rel),
            send_sem=x_send.at[0],
            recv_sem=x_recv.at[rel % NZ],
            device_id=partner,
            device_id_type=MESH,
        ).wait_recv()

    x_copies = []
    for k in range(NEAR, 0, -1):
        for s in (k, -k):
            copy = send_x(0, s, len(x_copies))
            copy.start()
            x_copies.append(copy)

    w_copies = []
    for i, (src, dst) in enumerate(
        [
            (gain_hbm, gb.at[own_d]),
            (wg_hbm.at[:, other_half], wgu.at[own_d, 0:FH]),
            (wu_hbm.at[:, other_half], wgu.at[own_d, FH:FL]),
            (wd_hbm.at[other_half, :], wd.at[:, own_d]),
        ]
    ):
        copy = pltpu.make_async_remote_copy(
            src_ref=src,
            dst_ref=dst,
            send_sem=bar_w_send.at[i],
            recv_sem=bar_w_recv.at[i],
            device_id=partner,
            device_id_type=MESH,
        )
        copy.start()
        w_copies.append(copy)

    arrive_x(-NEAR)
    for k in range(NEAR, 0, -1):
        copy = send_x(-NEAR, k, len(x_copies))
        copy.start()
        x_copies.append(copy)
    arrive_x(NEAR)
    for k in range(NEAR - 1, 0, -1):
        copy = send_x(NEAR, -k, len(x_copies))
        copy.start()
        x_copies.append(copy)

    def to_partner(g):
        rows = slice(g * GT, (g + 1) * GT)
        return pltpu.make_async_remote_copy(
            src_ref=xb.at[c, rows],
            dst_ref=xb.at[c, rows],
            send_sem=xd_send.at[g],
            recv_sem=xd_recv.at[g],
            device_id=partner,
            device_id_type=MESH,
        )

    def gate_up(g):
        rows = slice(g * GT, (g + 1) * GT)
        acc = None
        squares = None
        for h in range(2):
            values = xb[h, rows, :].astype(jnp.float32)
            part = jnp.sum(values * values, axis=1, keepdims=True)
            squares = part if squares is None else squares + part
            scaled = values * gb[h * DL : (h + 1) * DL].astype(jnp.float32)[None, :]
            high = scaled.astype(jnp.bfloat16)
            low = (scaled - high.astype(jnp.float32)).astype(jnp.bfloat16)
            w = wgu[h * DL : (h + 1) * DL, :]
            for lhs in (high, low):
                part = jnp.dot(lhs, w, preferred_element_type=jnp.float32)
                acc = part if acc is None else acc + part
        pb[g, :, :, 0:FL] = acc.reshape(NO, OT, FL).astype(jnp.bfloat16)
        sq_high = squares.astype(jnp.bfloat16).astype(jnp.float32)
        sq_low = squares - sq_high
        lane = lax.broadcasted_iota(jnp.int32, (GT, 128), 1)
        lanes = jnp.where(lane == 0, sq_high, jnp.where(lane == 1, sq_low, 0.0))
        pb[g, :, :, FL:PW] = lanes.reshape(NO, OT, 128).astype(jnp.bfloat16)

    def send_parts(g):
        copies = []
        for d in (10, 6, 14, 9, 11, 2, 8, 5, 7, 13, 15, 1, 3, 4, 12):
            peer = in_plane(d)
            copy = pltpu.make_async_remote_copy(
                src_ref=pb.at[g, peer[0] * 4 + peer[1]],
                dst_ref=rb.at[g, d - 1],
                send_sem=p_send.at[g * NO + d],
                recv_sem=p_recv.at[g * NO + d],
                device_id=peer,
                device_id_type=MESH,
            )
            copy.start()
            copies.append(copy)
        return copies

    def hidden(g, copies):
        for copy in copies:
            copy.wait_recv()
        total = pb[g, me].astype(jnp.float32)
        for d in range(NO - 1):
            total = total + rb[g, d].astype(jnp.float32)
        mean_sq = jnp.sum(total[:, FL:PW], axis=1, keepdims=True) / (DL * 32)
        scale = lax.rsqrt(mean_sq + EPS)
        gate = total[:, 0:FH] * scale
        up = total[:, FH:FL] * scale
        hb[g, me] = (gate / (1.0 + jnp.exp(-gate)) * up).astype(jnp.bfloat16)

    def send_hidden(g):
        copies = []
        for d in (10, 6, 14, 9, 11, 2, 8, 5, 7, 13, 15, 1, 3, 4, 12):
            copy = pltpu.make_async_remote_copy(
                src_ref=hb.at[g, me],
                dst_ref=hb.at[g, me],
                send_sem=h_send.at[g * NO + d],
                recv_sem=h_recv.at[g * NO + d],
                device_id=in_plane(d),
                device_id_type=MESH,
            )
            copy.start()
            copies.append(copy)
        return copies

    def down(g, copies):
        for copy in copies:
            copy.wait_recv()
        lhs = hb[g].astype(jnp.float32).reshape(GT, FH).astype(jnp.bfloat16)
        part = jnp.dot(lhs, wd[...], preferred_element_type=jnp.float32)
        db[g, 0] = part[:, 0:DL]
        db[g, 1] = part[:, DL:]
        copy = pltpu.make_async_remote_copy(
            src_ref=db.at[g, other],
            dst_ref=de.at[g],
            send_sem=d_send.at[g],
            recv_sem=d_recv.at[g],
            device_id=partner,
            device_id_type=MESH,
        )
        copy.start()
        return copy

    def send_home(g, copy):
        copy.wait_recv()
        total = db[g, c] + de[g]
        zs[g * 8 : (g + 1) * 8] = total.reshape(8, TB, DL).astype(jnp.bfloat16)
        copies = []
        rels = [r for r in range(-7, 9) if place(r) // 8 == g and r != 0]
        for r in sorted(rels, key=lambda r: -abs(r)):
            copy = pltpu.make_async_remote_copy(
                src_ref=zs.at[place(r)],
                dst_ref=zb.at[(-r) % NZ],
                send_sem=z_send.at[r % NZ],
                recv_sem=z_recv.at[(-r) % NZ],
                device_id=at_z(r),
                device_id_type=MESH,
            )
            copy.start()
            copies.append(copy)
        return copies

    for r in range(-HOME, NEAR):
        if r != 0:
            arrive_x(r)
    d_copies = [to_partner(0), to_partner(1)]
    d_copies[0].start()
    for copy in loads[1:]:
        copy.wait()
    for copy in w_copies:
        copy.wait_recv()
    d_copies[0].wait_recv()
    gate_up(0)
    parts = [send_parts(0)]

    for r in range(NEAR + 1, NEAR + 8):
        arrive_x(r)
    d_copies[1].start()
    d_copies[1].wait_recv()
    gate_up(1)
    parts.append(send_parts(1))

    hiddens = []
    for g in range(2):
        hidden(g, parts[g])
        hiddens.append(send_hidden(g))

    downs = []
    homes = []
    for g in range(2):
        downs.append(down(g, hiddens[g]))
    for g in range(2):
        homes += send_home(g, downs[g])

    total = zs[HOME].astype(jnp.float32)
    for r in range(1, NZ):
        pltpu.make_async_remote_copy(
            src_ref=zb.at[r],
            dst_ref=zb.at[r],
            send_sem=z_send.at[0],
            recv_sem=z_recv.at[r],
            device_id=partner,
            device_id_type=MESH,
        ).wait_recv()
    for r in range(1, NZ):
        total = total + zb[r].astype(jnp.float32)
    out_ref[...] = total.astype(jnp.bfloat16)

    for copy in x_copies + w_copies + d_copies + parts[0] + parts[1] + hiddens[0] + hiddens[1] + downs + homes:
        copy.wait_send()


def per_device(patches, norm_gain, gate_weight, up_weight, down_weight):
    bf16, f32 = jnp.bfloat16, jnp.float32
    dma = pltpu.SemaphoreType.DMA
    return pl.pallas_call(
        kernel,
        out_shape=jax.ShapeDtypeStruct((TB, DL), bf16),
        in_specs=[pl.BlockSpec(memory_space=pltpu.HBM)] * 5,
        out_specs=pl.BlockSpec(memory_space=pltpu.VMEM),
        scratch_shapes=[
            pltpu.VMEM((2, NZ * TB, DL), bf16),
            pltpu.VMEM((2 * DL,), bf16),
            pltpu.VMEM((2 * DL, FL), bf16),
            pltpu.VMEM((FH, 2 * DL), bf16),
            pltpu.VMEM((2, NO, OT, PW), bf16),
            pltpu.VMEM((2, NO - 1, OT, PW), bf16),
            pltpu.VMEM((2, NO, OT, FH), bf16),
            pltpu.VMEM((2, 2, GT, DL), f32),
            pltpu.VMEM((2, GT, DL), f32),
            pltpu.VMEM((NZ, TB, DL), bf16),
            pltpu.VMEM((NZ, TB, DL), bf16),
            dma((5,)),
            dma((4,)), dma((4,)),
            dma((15,)), dma((NZ,)),
            dma((2,)), dma((2,)),
            dma((2 * NO,)), dma((2 * NO,)),
            dma((2 * NO,)), dma((2 * NO,)),
            dma((2,)), dma((2,)),
            dma((NZ,)), dma((NZ,)),
        ],
        compiler_params=pltpu.CompilerParams(
            collective_id=0, has_side_effects=True, vmem_limit_bytes=67043328
        ),
    )(patches, norm_gain, gate_weight, up_weight, down_weight)


def solution(mesh):
    torus = Mesh(mesh.devices.reshape(4, 4, 2, mesh.shape["gy"]), ("gx_0", "gx_1", "gx_2", "gy"))
    in_specs = (P("gy", GX), P(GX), P(GX, "gy"), P(GX, "gy"), P("gy", GX))
    out_specs = P("gy", GX)
    return jax.shard_map(
        per_device, mesh=torus, in_specs=in_specs, out_specs=out_specs, check_vma=False
    )
```
